32 devices in a mesh: section: 4 (over z), gx: 2 (over x), gy: 2 (over y), gz: 2 (over core).
Axes of the slice: x: 2, y: 2, z: 4, core: 2. Of those that a mesh axis runs over, the one named last changes fastest.
Arguments:
- micro_inputs: bfloat16 [1, 256, 8192], P(None, 'gy', ('gx', 'gz')), may hold values from -40 to 40
- norm_gain: float32 [4, 8192], P('section', 'gx'), may hold values from 0.5 to 1.5
- q_weight: bfloat16 [4, 8192, 8192], P('section', ('gx', 'gy'), 'gz'), may hold values from -0.0625 to 0.0625
- kv_weight: bfloat16 [4, 2, 8192, 1024], P('section', None, ('gx', 'gy'), 'gz'), may hold values from -0.0625 to 0.0625
- q_bias: float32 [4, 8192], P('section', 'gz'), may hold values from -130 to 130
- kv_bias: float32 [4, 2, 1024], P('section', None, 'gz'), may hold values from -50 to 50
- out_weight: bfloat16 [4, 8192, 8192], P('section', 'gz', ('gx', 'gy')), may hold values from -0.0625 to 0.0625
Outputs:
- hidden_out: bfloat16 [4, 1, 256, 8192], P('section', None, 'gy', ('gx', 'gz'))
The draws below stay inside these ranges and needn't reach their ends.
All inputs are finite; a program needn't handle non-finite values.
Results may differ from the reference program's by a relative error of at most 0.025.
Values may be sent and summed in bfloat16 or wider, within the bound.
No kernel may reach another device: no remote copies, remote signals or barrier semaphores. Data moves between devices by JAX's collectives and lax.ppermute only.
A program may use at most 128 MiB of HBM per device.

```python
import math
import jax
import jax.numpy as jnp
from jax import lax

D = 8192
HQ = 64
KV = 8
HD = 128
SEQ = 256
MICRO = 1
LAYERS = 4


def draw_micro_inputs(key, part):
    noise_key, row_key, col_key = jax.random.split(key, 3)
    values = jax.random.normal(noise_key, (MICRO, SEQ, D), jnp.float32)
    rising = jnp.exp(math.log(3.0) * jnp.arange(D, dtype=jnp.float32) / (D - 1))
    row_scale = jnp.exp(jax.random.uniform(row_key, (MICRO, SEQ, 1), jnp.float32, -0.4, 0.4))
    col_scale = jnp.exp(jax.random.uniform(col_key, (D,), jnp.float32, -0.4, 0.4)) * rising / 1.8
    return jnp.clip(values * row_scale * col_scale[None, None, :], -40.0, 40.0).astype(jnp.bfloat16)


def draw_q_bias(key, part):
    noise = jnp.clip(0.5 * jax.random.normal(jax.random.fold_in(key, 21), (LAYERS, HQ * HD), jnp.float32), -2.0, 2.0)
    return noise


def draw_kv_bias(key, part):
    noise = jnp.clip(0.5 * jax.random.normal(jax.random.fold_in(key, 22), (LAYERS, 2, KV * HD), jnp.float32), -2.0, 2.0)
    return noise


def shard_levels(own_key, dims, cuts, smallest, largest):
    loudness, own = 1.0, jax.random.fold_in(own_key, 6)
    for position, parts in cuts:
        heights = jnp.exp(jax.random.uniform(jax.random.fold_in(own, position), (parts,), jnp.float32, smallest / len(cuts), largest / len(cuts)))
        loudness = loudness * jnp.repeat(heights, dims[position] // parts).reshape([-1 if axis == position else 1 for axis in range(len(dims))])
    return loudness


def centred(own_key, dims, deviation, bound, cuts=(), held_as=jnp.bfloat16):
    entries = deviation * jax.random.normal(own_key, dims, jnp.float32)
    if cuts:
        entries = entries * shard_levels(own_key, dims, cuts, -0.22, 0.18)
    return jnp.clip(entries, -bound, bound).astype(held_as)


def setup_inputs(seed: int = 0) -> dict:
    key_list = jax.random.split(jax.random.key(seed), 8)
    return {
        "micro_inputs": draw_micro_inputs(jax.random.fold_in(key_list[7], 71), 0),
        "norm_gain": jnp.clip(1.0 + 0.1 * jax.random.normal(key_list[1], (LAYERS, D), jnp.float32), 0.5, 1.5),
        "q_weight": centred(key_list[2], (LAYERS, D, HQ * HD), D ** -0.5, 0.0625, ((0, 4), (1, 4), (2, 2))),
        "kv_weight": centred(key_list[3], (LAYERS, 2, D, KV * HD), D ** -0.5, 0.0625, ((0, 4), (2, 4), (3, 2))),
        "q_bias": draw_q_bias(jax.random.fold_in(key_list[7], 71), 0),
        "kv_bias": draw_kv_bias(jax.random.fold_in(key_list[7], 71), 0),
        "out_weight": centred(key_list[6], (LAYERS, HQ * HD, D), (HQ * HD) ** -0.5, 0.0625, ((0, 4), (1, 2), (2, 4))),
    }


ROPE_BASE = 1000000.0
EPSILON = 1e-06
NEG_FILL = -1e+30

def rotary(values, positions):
    half_width = values.shape[-1] // 2
    frequency = ROPE_BASE ** (-jnp.arange(half_width, dtype=jnp.float32) * 2.0 / values.shape[-1])
    angles = positions.astype(jnp.float32)[:, None] * frequency[None, :]
    cosine = jnp.cos(angles)[:, None, :]
    sine_part = jnp.sin(angles)[:, None, :]
    lower_half = values[..., :half_width]
    upper_half = values[..., half_width:]
    return jnp.concatenate([lower_half * cosine - upper_half * sine_part, upper_half * cosine + lower_half * sine_part], axis=-1)

def reference(micro_inputs, norm_gain, q_weight, kv_weight, q_bias, kv_bias, out_weight):
    group_size = HQ // KV
    positions = jnp.arange(SEQ).astype(jnp.int32)
    causal = positions[None, :] <= positions[:, None]
    score_scale = HD ** (-0.5)

    def one_layer(hidden, layer):
        widened = hidden.astype(jnp.float32)
        mean_square = lax.optimization_barrier(jnp.mean(widened * widened, axis=1))
        normed = (widened * lax.rsqrt(mean_square + EPSILON)[:, None] * norm_gain[layer][None, :]).astype(jnp.bfloat16)
        queries = jnp.dot(normed, q_weight[layer], preferred_element_type=jnp.float32) + q_bias[layer][None, :]
        key_rows = jnp.dot(normed, kv_weight[layer, 0], preferred_element_type=jnp.float32) + kv_bias[layer, 0][None, :]
        value_rows = jnp.dot(normed, kv_weight[layer, 1], preferred_element_type=jnp.float32) + kv_bias[layer, 1][None, :]
        queries = lax.optimization_barrier(rotary(queries.reshape(SEQ, HQ, HD), positions).astype(jnp.bfloat16))
        key_rows = lax.optimization_barrier(rotary(key_rows.reshape(SEQ, KV, HD), positions).astype(jnp.bfloat16))
        value_rows = lax.optimization_barrier(value_rows.reshape(SEQ, KV, HD).astype(jnp.bfloat16))
        grouped = queries.reshape(SEQ, KV, group_size, HD).astype(jnp.float32)
        scores = jnp.einsum('qhgd,khd->hgqk', grouped, key_rows.astype(jnp.float32)) * score_scale
        scores = jnp.where(causal, scores, NEG_FILL)
        peak = lax.optimization_barrier(jnp.max(scores, axis=-1, keepdims=True))
        weights = jnp.where(causal, jnp.exp(scores - peak), 0.0)
        total = lax.optimization_barrier(jnp.sum(weights, axis=-1))
        rounded = lax.optimization_barrier(weights.astype(jnp.bfloat16)).astype(jnp.float32)
        mixed = jnp.einsum('hgqk,khd->qhgd', rounded, value_rows.astype(jnp.float32))
        attended = (mixed / jnp.transpose(total, (2, 0, 1))[..., None]).astype(jnp.bfloat16).reshape(SEQ, HQ * HD)
        branch = jnp.dot(attended, out_weight[layer], preferred_element_type=jnp.float32)
        return (widened + branch).astype(jnp.bfloat16)
    results = []
    for micro in range(MICRO):
        hidden = micro_inputs[micro]
        per_layer = []
        for layer in range(LAYERS):
            hidden = one_layer(hidden, layer)
            per_layer.append(hidden)
        results.append(jnp.stack(per_layer))
    return jnp.stack(results, axis=1)
```

```python
import jax
import jax.numpy as jnp
from jax import lax
from jax.sharding import PartitionSpec as P

HD = 128
ROPE_BASE = 1000000.0
EPSILON = 1e-06
NEG_FILL = -1e30
CHUNKS = 2


def body(micro_inputs, norm_gain, q_weight, kv_weight, q_bias, kv_bias, out_weight):
    sections = lax.axis_size("section")
    size_gx, size_gy, size_gz = (lax.axis_size(a) for a in ("gx", "gy", "gz"))
    group = size_gx * size_gy
    index_gx, index_gy, index_gz = (lax.axis_index(a) for a in ("gx", "gy", "gz"))
    index_section = lax.axis_index("section")
    me = index_gx * size_gy + index_gy
    micro_count = micro_inputs.shape[0]
    tokens = micro_inputs.shape[1] * size_gy
    width = micro_inputs.shape[2] * size_gx * size_gz
    slab = q_weight.shape[1]
    chunk = tokens // CHUNKS
    share = chunk // size_gz
    query_weight = q_weight[0]
    key_weight = kv_weight[0, 0]
    value_weight = kv_weight[0, 1]
    mixing_weight = out_weight[0]
    q_cols = query_weight.shape[1]
    kv_cols = key_weight.shape[1]
    group_size = q_cols // kv_cols
    own_cols = q_cols // group
    own_heads = own_cols // HD
    used_heads = max(1, own_heads // group_size)
    used_cols = used_heads * HD
    local_group = own_heads // used_heads
    score_scale = HD ** (-0.5)

    offsets = [(dx, dy) for dx in range(size_gx) for dy in range(size_gy)]
    offsets = sorted(offsets[1:], key=lambda o: -(min(o[0], size_gx - o[0]) + min(o[1], size_gy - o[1])))

    def chip_at(dx, dy):
        return (index_gx + dx) % size_gx * size_gy + (index_gy + dy) % size_gy

    def to_offset(value, dx, dy):
        pairs = [
            (x * size_gy + y, (x + dx) % size_gx * size_gy + (y + dy) % size_gy)
            for x in range(size_gx)
            for y in range(size_gy)
        ]
        return lax.ppermute(value, ("gx", "gy"), pairs)

    def around(value, axis, steps):
        count = lax.axis_size(axis)
        return lax.ppermute(value, axis, [(i, (i + steps) % count) for i in range(count)])

    def kv_start(chip):
        return chip * own_heads // group_size * HD

    gain_slab = lax.dynamic_slice_in_dim(norm_gain[0], index_gy * slab, slab, 0)
    own_q_bias = lax.dynamic_slice_in_dim(q_bias[0], me * own_cols, own_cols, 0)
    own_k_bias = lax.dynamic_slice_in_dim(kv_bias[0, 0], kv_start(me), used_cols, 0)
    own_v_bias = lax.dynamic_slice_in_dim(kv_bias[0, 1], kv_start(me), used_cols, 0)

    order = (index_gz + jnp.arange(size_gz)) % size_gz
    row_pos = (order[:, None] * share + jnp.arange(share)[None, :]).reshape(chunk)
    half_width = HD // 2
    frequency = ROPE_BASE ** (-jnp.arange(half_width, dtype=jnp.float32) * 2.0 / HD)
    all_pos = (jnp.arange(CHUNKS)[:, None] * chunk + row_pos[None, :]).reshape(-1)
    angles = all_pos.astype(jnp.float32)[:, None] * frequency[None, :]
    cosines = jnp.cos(angles).reshape(CHUNKS, chunk, half_width)
    sines = jnp.sin(angles).reshape(CHUNKS, chunk, half_width)

    def rotary(values, cosine, sine):
        lower, upper = values[..., :half_width], values[..., half_width:]
        cosine, sine = cosine[:, None, :], sine[:, None, :]
        return jnp.concatenate([lower * cosine - upper * sine, upper * cosine + lower * sine], axis=-1)

    def project(scaled, chip):
        q_part = jnp.dot(
            scaled,
            lax.dynamic_slice_in_dim(query_weight, chip * own_cols, own_cols, 1),
            preferred_element_type=jnp.float32,
        )
        k_part = jnp.dot(
            scaled,
            lax.dynamic_slice_in_dim(key_weight, kv_start(chip), used_cols, 1),
            preferred_element_type=jnp.float32,
        )
        v_part = jnp.dot(
            scaled,
            lax.dynamic_slice_in_dim(value_weight, kv_start(chip), used_cols, 1),
            preferred_element_type=jnp.float32,
        )
        return jnp.concatenate([q_part, k_part, v_part], axis=1)

    def mix(block, chip):
        return jnp.dot(
            block,
            lax.dynamic_slice_in_dim(mixing_weight, chip * own_cols, own_cols, 0),
            preferred_element_type=jnp.float32,
        )

    def layer(own_rows, ordinal, earlier):
        rows = [own_rows] + [around(own_rows, "gz", -j) for j in range(1, size_gz)]
        wide = jnp.concatenate(rows, axis=0).astype(jnp.float32)
        scaled = (wide * gain_slab[None, :]).astype(jnp.bfloat16)
        total = jnp.sum(wide * wide, axis=1)
        sums = total
        received = []
        for dx, dy in offsets:
            part = project(scaled, chip_at(dx, dy)).astype(jnp.bfloat16)
            received.append(to_offset(part, dx, dy))
        for dx, dy in offsets:
            sums = sums + to_offset(total, dx, dy)
        projected = project(scaled, me)
        for part in received:
            projected = projected + part.astype(jnp.float32)
        projected = projected * lax.rsqrt(sums / width + EPSILON)[:, None]
        clipped = jnp.clip(ordinal, 0, CHUNKS - 1)
        cosine = lax.dynamic_index_in_dim(cosines, clipped, 0, keepdims=False)
        sine = lax.dynamic_index_in_dim(sines, clipped, 0, keepdims=False)
        queries = (projected[:, :own_cols] + own_q_bias[None, :]).reshape(chunk, own_heads, HD)
        keys = (projected[:, own_cols : own_cols + used_cols] + own_k_bias[None, :]).reshape(chunk, used_heads, HD)
        values = (projected[:, own_cols + used_cols :] + own_v_bias[None, :]).reshape(chunk, used_heads, HD)
        queries = rotary(queries, cosine, sine).astype(jnp.bfloat16)
        keys = rotary(keys, cosine, sine).astype(jnp.bfloat16)
        values = values.astype(jnp.bfloat16)
        seen = ([(keys, values)] + earlier)[:CHUNKS]
        all_keys = jnp.concatenate([k for k, _ in seen], axis=0)
        all_values = jnp.concatenate([v for _, v in seen], axis=0)
        allowed = jnp.concatenate(
            [row_pos[None, :] <= row_pos[:, None]]
            + [jnp.broadcast_to(ordinal >= j, (chunk, chunk)) for j in range(1, len(seen))],
            axis=1,
        )
        scores = (
            jnp.einsum(
                "qhgd,khd->hgqk",
                queries.reshape(chunk, used_heads, local_group, HD),
                all_keys,
                preferred_element_type=jnp.float32,
            )
            * score_scale
        )
        scores = jnp.where(allowed, scores, NEG_FILL)
        weights = jnp.where(allowed, jnp.exp(scores - jnp.max(scores, axis=-1, keepdims=True)), 0.0)
        denominators = jnp.sum(weights, axis=-1)
        weighted = jnp.einsum(
            "hgqk,khd->qhgd", weights.astype(jnp.bfloat16), all_values, preferred_element_type=jnp.float32
        )
        attended = (
            (weighted / jnp.transpose(denominators, (2, 0, 1))[..., None]).astype(jnp.bfloat16).reshape(chunk, own_cols)
        )
        arrived = [(chip_at(-dx, -dy), to_offset(attended, dx, dy)) for dx, dy in offsets]
        column_sums = mix(attended, me)
        for chip, block in reversed(arrived):
            column_sums = column_sums + mix(block, chip)
        own_sum = column_sums[:share].astype(jnp.bfloat16).astype(jnp.float32)
        for j in range(1, size_gz):
            piece = column_sums[j * share : (j + 1) * share].astype(jnp.bfloat16)
            own_sum = own_sum + around(piece, "gz", j).astype(jnp.float32)
        result = (own_rows.astype(jnp.float32) + own_sum).astype(jnp.bfloat16)
        return result, seen

    def gathered(value, axis, dim):
        pieces = [value] + [around(value, axis, -j) for j in range(1, lax.axis_size(axis))]
        stacked = jnp.stack(pieces)
        count = lax.axis_size(axis)
        stacked = jnp.take(stacked, (jnp.arange(count) - lax.axis_index(axis)) % count, axis=0)
        moved = jnp.moveaxis(stacked, 0, dim)
        shape = list(value.shape)
        shape[dim] *= count
        return moved.reshape(shape)

    def spread(block):
        wide = gathered(block, "gz", 1)
        pieces = lax.all_to_all(wide, "gy", split_axis=1, concat_axis=0, tiled=True)
        pieces = pieces.reshape(CHUNKS, size_gz, share, slab)
        return lax.dynamic_index_in_dim(pieces, index_gz, 1, keepdims=False)

    fresh = [spread(micro_inputs[m]) for m in range(micro_count)]
    entering = [fresh[m][c] for m in range(micro_count) for c in range(CHUNKS)]
    jobs = micro_count * CHUNKS
    stored = jnp.zeros((jobs, share, slab), jnp.bfloat16)
    carried = entering[0]
    earlier = []
    for tick in range(jobs + sections - 1):
        job = tick - index_section
        ordinal = job % CHUNKS
        current = jnp.where(index_section == 0, entering[tick], carried) if tick < jobs else carried
        result, earlier = layer(current, ordinal, earlier)
        valid = (job >= 0) & (job < jobs)
        spot = jnp.clip(job, 0, jobs - 1)
        previous = lax.dynamic_index_in_dim(stored, spot, 0, keepdims=False)
        stored = lax.dynamic_update_index_in_dim(stored, jnp.where(valid, result, previous), spot, 0)
        if tick < jobs + sections - 2:
            carried = lax.ppermute(result, "section", [(i, i + 1) for i in range(sections - 1)])

    def collect(slabs):
        rows = gathered(slabs, "gz", 1)
        rows = rows.reshape(tokens, slab)
        wide = lax.all_to_all(rows, "gy", split_axis=0, concat_axis=1, tiled=True)
        piece = wide.shape[1] // size_gz
        return lax.dynamic_slice_in_dim(wide, index_gz * piece, piece, 1)

    stored = stored.reshape(micro_count, CHUNKS, share, slab)
    return jnp.stack([collect(stored[m]) for m in range(micro_count)])[None]


def solution(mesh):
    return jax.shard_map(
        body,
        mesh=mesh,
        in_specs=(
            P(None, "gy", ("gx", "gz")),
            P("section", "gx"),
            P("section", ("gx", "gy"), "gz"),
            P("section", None, ("gx", "gy"), "gz"),
            P("section", "gz"),
            P("section", None, "gz"),
            P("section", "gz", ("gx", "gy")),
        ),
        out_specs=P("section", None, "gy", ("gx", "gz")),
        check_vma=False,
    )
```

```python
import jax
import jax.numpy as jnp
from jax import lax
from jax.experimental import pallas as pl
from jax.experimental.pallas import tpu as pltpu
from jax.sharding import PartitionSpec as P

HD = 128
ROPE_BASE = 1000000.0
EPSILON = 1e-06
NEG_FILL = -1e30
CHUNKS = 2
HELD_BLOCKS = 3
WHOLE = pl.BlockSpec(memory_space=pltpu.VMEM)
SCALARS = pl.BlockSpec(memory_space=pltpu.SMEM)
LIMIT = pltpu.CompilerParams(vmem_limit_bytes=4 << 20)


def tile_of(columns):
    return 256 if columns % 256 == 0 else 128


def effort(flops, moved=0):
    return pl.CostEstimate(flops=flops, transcendentals=0, bytes_accessed=moved)


def resident(small, early, sources, copies, shapes):
    def kernel(*refs):
        small_refs = refs[: len(small)]
        source_refs = refs[len(small) : len(small) + len(sources)]
        outs = refs[len(small) + len(sources) + len(early) :]
        moves = []
        for i, (source, where, held, target) in enumerate(copies):
            where = where(small_refs[0]) if callable(where) else where
            moves.append(
                pltpu.make_async_copy(source_refs[source].at[where], outs[len(small) + held].at[target], outs[-1].at[i])
            )
        for move in moves:
            move.start()
        for value, ref, out in zip(small, small_refs, outs):
            if value.dtype == jnp.int32:
                for i in range(value.shape[0]):
                    out[i] = ref[i]
            else:
                out[...] = ref[...]
        for move in moves:
            move.wait()

    def space(value):
        return SCALARS if value.dtype == jnp.int32 else WHOLE

    return pl.pallas_call(
        kernel,
        out_shape=[(pltpu.SMEM if v.dtype == jnp.int32 else pltpu.VMEM)(v.shape, v.dtype) for v in small]
        + [pltpu.VMEM(shape, jnp.bfloat16) for shape in shapes],
        in_specs=[space(v) for v in small] + [pl.BlockSpec(memory_space=pltpu.HBM)] * len(sources)
        + [pl.BlockSpec(memory_space=pl.ANY)] * len(early),
        out_specs=[space(v) for v in small] + [WHOLE] * len(shapes),
        scratch_shapes=[pltpu.SemaphoreType.DMA((len(copies),))],
        compiler_params=pltpu.CompilerParams(vmem_limit_bytes=1 << 20),
        cost_estimate=effort(1 << 32),
    )(*small, *[pltpu.with_memory_space_constraint(x, pltpu.HBM) for x in sources], *early)


def project_into(o_ref, x_ref, w_ref, start, width):
    tile = tile_of(width)

    def step(i, _):
        o_ref[:, pl.ds(pl.multiple_of(i * tile, 128), tile)] = jnp.dot(
            x_ref[...],
            w_ref[:, pl.ds(pl.multiple_of(start + i * tile, 128), tile)],
            preferred_element_type=jnp.float32,
        ).astype(o_ref.dtype)
        return 0

    lax.fori_loop(0, width // tile, step, 0)


def project_block(table, slot, rows, weight, width, kind):
    def kernel(table_ref, x_ref, w_ref, o_ref):
        project_into(o_ref, x_ref, w_ref, table_ref[slot] * width, width)

    return pl.pallas_call(
        kernel,
        out_shape=jax.ShapeDtypeStruct((rows.shape[0], width), kind),
        in_specs=[SCALARS, WHOLE, WHOLE],
        out_specs=WHOLE,
        compiler_params=LIMIT,
        cost_estimate=effort(2 * rows.shape[0] * rows.shape[1] * width),
    )(table, rows, weight)


def enter(table, slot, pieces, gain, weight, width):
    count = len(pieces)
    share, slab = pieces[0].shape
    chunk = share * count

    def kernel(table_ref, gain_ref, w_ref, *refs):
        scaled_ref, total_ref, o_ref = refs[count:]
        totals = []
        for i in range(count):
            wide = refs[i][...].astype(jnp.float32)
            scaled_ref[i * share : (i + 1) * share, :] = (wide * gain_ref[...]).astype(jnp.bfloat16)
            totals.append(jnp.sum(wide * wide, axis=1, keepdims=True))
        total = jnp.broadcast_to(jnp.concatenate(totals, axis=0), (chunk, 128))
        total_ref[...] = jnp.transpose(total)[:8]
        project_into(o_ref, scaled_ref, w_ref, table_ref[slot] * width, width)

    return pl.pallas_call(
        kernel,
        out_shape=(
            jax.ShapeDtypeStruct((chunk, slab), jnp.bfloat16),
            jax.ShapeDtypeStruct((8, chunk), jnp.float32),
            jax.ShapeDtypeStruct((chunk, width), jnp.bfloat16),
        ),
        in_specs=[SCALARS] + [WHOLE] * (2 + count),
        out_specs=(WHOLE, WHOLE, WHOLE),
        compiler_params=LIMIT,
        cost_estimate=effort(2 * chunk * slab * width),
    )(table, gain, weight, *pieces)


def attend(projected, received, totals, bias, cosine, sine, mask, earlier, heads, used, features):
    chunk = projected.shape[0]
    group = heads // used
    own_cols = heads * HD
    used_cols = used * HD
    parts = len(received)
    past = len(earlier)
    scale = HD ** (-0.5)

    def kernel(p_ref, bias_ref, cos_ref, sin_ref, mask_ref, *refs):
        part_refs = refs[:parts]
        total_refs = refs[parts : 2 * parts + 1]
        past_refs = refs[2 * parts + 1 : 2 * parts + 1 + 2 * past]
        o_ref, k_ref, v_ref = refs[2 * parts + 1 + 2 * past :]
        total = total_refs[0][0:1, :]
        for ref in total_refs[1:]:
            total = total + ref[0:1, :]
        inverse = lax.rsqrt(total / features + EPSILON)
        inverse = jnp.transpose(jnp.broadcast_to(inverse, (HD, chunk)))
        cosine_rows = cos_ref[...]
        sine_rows = sin_ref[...]

        def columns(start):
            value = p_ref[:, start : start + HD]
            for ref in part_refs:
                value = value + ref[:, start : start + HD].astype(jnp.float32)
            return value * inverse + bias_ref[:, start : start + HD]

        def rotate(value):
            return (value * cosine_rows + pltpu.roll(value, HD // 2, 1) * sine_rows).astype(jnp.bfloat16)

        allowed = mask_ref[...] > 0.5
        for u in range(used):
            spot = slice(u * HD, (u + 1) * HD)
            k_ref[:, spot] = rotate(columns(own_cols + u * HD))
            v_ref[:, spot] = columns(own_cols + used_cols + u * HD).astype(jnp.bfloat16)
            keys = [k_ref[:, spot]] + [past_refs[2 * j][:, spot] for j in range(past)]
            values = [v_ref[:, spot]] + [past_refs[2 * j + 1][:, spot] for j in range(past)]
            keys = jnp.concatenate(keys, axis=0) if past else keys[0]
            values = jnp.concatenate(values, axis=0) if past else values[0]
            for g in range(group):
                start = (u * group + g) * HD
                query = rotate(columns(start))
                scores = (
                    lax.dot_general(query, keys, (((1,), (1,)), ((), ())), preferred_element_type=jnp.float32) * scale
                )
                scores = jnp.where(allowed, scores, NEG_FILL)
                weights = jnp.where(allowed, jnp.exp(scores - jnp.max(scores, axis=1, keepdims=True)), 0.0)
                denominator = jnp.sum(weights, axis=1, keepdims=True)
                mixed = jnp.dot(weights.astype(jnp.bfloat16), values, preferred_element_type=jnp.float32)
                o_ref[:, start : start + HD] = (mixed / denominator).astype(jnp.bfloat16)

    return pl.pallas_call(
        kernel,
        out_shape=(
            jax.ShapeDtypeStruct((chunk, own_cols), jnp.bfloat16),
            jax.ShapeDtypeStruct((chunk, used_cols), jnp.bfloat16),
            jax.ShapeDtypeStruct((chunk, used_cols), jnp.bfloat16),
        ),
        in_specs=[WHOLE] * (5 + 2 * parts + 1 + 2 * past),
        out_specs=(WHOLE, WHOLE, WHOLE),
        compiler_params=LIMIT,
        cost_estimate=effort(1 << 29),
    )(projected, bias, cosine, sine, mask, *received, *totals, *[a for pair in earlier for a in pair])


def mix_blocks(table, slots, blocks, weight, held, so_far, cores):
    count = len(blocks)
    chunk, depth = blocks[0].shape
    slab = weight.shape[2]
    share = chunk // cores
    tile = min(slab, 512)
    near = [b for b in range(count) if slots[b] in held]
    steps = [(i, b) for i in range(slab // tile) for b in range(count) if b not in near]
    buffers = min(4, len(steps))
    ready = [held[slots[b]] for b in near]
    inputs = [*blocks, *ready] + ([] if so_far is None else [so_far])

    def kernel(table_ref, w_ref, *refs):
        outs = refs[len(inputs) : len(inputs) + cores]
        fetches = []
        for step, (i, b) in enumerate(steps):
            row = pl.multiple_of(table_ref[slots[b]] * depth, 128)
            buffer, sems = refs[-2:]
            fetches.append(
                pltpu.make_async_copy(
                    w_ref.at[0, pl.ds(row, depth), pl.ds(i * tile, tile)],
                    buffer.at[step % buffers],
                    sems.at[step % buffers],
                )
            )
        for fetch in fetches[:buffers]:
            fetch.start()
        for i in range(slab // tile):
            spot = slice(i * tile, (i + 1) * tile)
            out = None if so_far is None else refs[len(inputs) - 1][:, spot]
            for b in near + [b for b in range(count) if b not in near]:
                if b in near:
                    rows = refs[count + near.index(b)][:, spot]
                else:
                    step = steps.index((i, b))
                    fetches[step].wait()
                    rows = refs[-2][step % buffers]
                term = jnp.dot(refs[b][...], rows, preferred_element_type=jnp.float32)
                out = term if out is None else out + term
                if b not in near and step + buffers < len(steps):
                    fetches[step + buffers].start()
            for j, ref in enumerate(outs):
                ref[:, spot] = out[j * share : (j + 1) * share].astype(ref.dtype)

    scratch = [pltpu.VMEM((buffers, depth, tile), jnp.bfloat16), pltpu.SemaphoreType.DMA((buffers,))]
    return pl.pallas_call(
        kernel,
        out_shape=[
            jax.ShapeDtypeStruct((share, slab), jnp.bfloat16 if j else jnp.float32) for j in range(cores)
        ],
        in_specs=[SCALARS, pl.BlockSpec(memory_space=pltpu.HBM)] + [WHOLE] * len(inputs),
        out_specs=[WHOLE] * cores,
        scratch_shapes=scratch if steps else [],
        compiler_params=pltpu.CompilerParams(vmem_limit_bytes=8 << 20),
        cost_estimate=effort(2 * count * chunk * depth * slab),
    )(table, weight, *inputs)


def leave(rows, own_sum, pieces):
    def kernel(x_ref, sum_ref, *refs):
        value = x_ref[...].astype(jnp.float32) + sum_ref[...]
        for ref in refs[:-1]:
            value = value + ref[...].astype(jnp.float32)
        refs[-1][...] = value.astype(jnp.bfloat16)

    return pl.pallas_call(
        kernel,
        out_shape=jax.ShapeDtypeStruct(rows.shape, jnp.bfloat16),
        in_specs=[WHOLE] * (2 + len(pieces)),
        out_specs=WHOLE,
        compiler_params=LIMIT,
        cost_estimate=effort(1 << 26),
    )(rows, own_sum, *pieces)


def around(value, axis, steps):
    count = lax.axis_size(axis)
    return lax.ppermute(value, axis, [(i, (i + steps) % count) for i in range(count)])


def gathered(value, axis, dim):
    pieces = [value] + [around(value, axis, -j) for j in range(1, lax.axis_size(axis))]
    count = lax.axis_size(axis)
    stacked = jnp.take(jnp.stack(pieces), (jnp.arange(count) - lax.axis_index(axis)) % count, axis=0)
    shape = list(value.shape)
    shape[dim] *= count
    return jnp.moveaxis(stacked, 0, dim).reshape(shape)


def body(micro_inputs, norm_gain, q_weight, kv_weight, q_bias, kv_bias, out_weight):
    sections = lax.axis_size("section")
    size_gx, size_gy, size_gz = (lax.axis_size(a) for a in ("gx", "gy", "gz"))
    group = size_gx * size_gy
    index_gx, index_gy, index_gz = (lax.axis_index(a) for a in ("gx", "gy", "gz"))
    index_section = lax.axis_index("section")
    me = index_gx * size_gy + index_gy
    micro_count = micro_inputs.shape[0]
    tokens = micro_inputs.shape[1] * size_gy
    features = micro_inputs.shape[2] * size_gx * size_gz
    slab = q_weight.shape[1]
    chunk = tokens // CHUNKS
    share = chunk // size_gz
    q_cols = q_weight.shape[2]
    kv_cols = kv_weight.shape[3]
    group_size = q_cols // kv_cols
    own_cols = q_cols // group
    own_heads = own_cols // HD
    used_heads = max(1, own_heads // group_size)
    used_cols = used_heads * HD
    width = own_cols + 2 * used_cols
    jobs = micro_count * CHUNKS

    offsets = [(dx, dy) for dx in range(size_gx) for dy in range(size_gy)][1:]
    offsets.sort(key=lambda o: (min(o[0], size_gx - o[0]) + min(o[1], size_gy - o[1])))

    def chip_at(dx, dy):
        x = index_gx + dx
        y = index_gy + dy
        return jnp.where(x >= size_gx, x - size_gx, x) * size_gy + jnp.where(y >= size_gy, y - size_gy, y)

    def to_offset(value, dx, dy):
        pairs = [
            (x * size_gy + y, (x + dx) % size_gx * size_gy + (y + dy) % size_gy)
            for x in range(size_gx)
            for y in range(size_gy)
        ]
        return lax.ppermute(value, ("gx", "gy"), pairs)

    def kv_start(chip):
        return chip * own_heads // group_size * HD

    even = size_gy == size_gz == CHUNKS
    if even:

        def spread(block):
            cut = block.reshape(size_gz, share, slab)
            pieces = []
            for j in range(CHUNKS):
                spot = lax.rem(index_gy + j, size_gz)
                pairs = [
                    (a * size_gz + b, b * size_gz + (a + j) % size_gz) for a in range(size_gy) for b in range(size_gz)
                ]
                piece = lax.dynamic_index_in_dim(cut, spot, 0, keepdims=False)
                pieces.append(lax.ppermute(piece, ("gy", "gz"), pairs))
            return [
                sum_of([(lax.rem(index_gz + size_gz - j, size_gz) == k, pieces[j]) for j in range(CHUNKS)])
                for k in range(CHUNKS)
            ]

        def collect(slabs):
            pieces = []
            for j in range(CHUNKS):
                pairs = [
                    (c * size_gz + d, (d + j) % size_gy * size_gz + c) for c in range(size_gy) for d in range(size_gz)
                ]
                piece = sum_of([(flag(sections + j * CHUNKS + k), slabs[k]) for k in range(CHUNKS)])
                pieces.append(lax.ppermute(piece, ("gy", "gz"), pairs))
            return jnp.concatenate(
                [
                    sum_of([(flag(sections + CHUNKS * CHUNKS + d * CHUNKS + j), pieces[j]) for j in range(CHUNKS)])
                    for d in range(size_gz)
                ],
                axis=0,
            )
    else:

        def spread(block):
            wide = gathered(block, "gz", 1)
            pieces = lax.all_to_all(wide, "gy", split_axis=1, concat_axis=0, tiled=True)
            pieces = pieces.reshape(CHUNKS, size_gz, share, slab)
            pieces = lax.dynamic_index_in_dim(pieces, index_gz, 1, keepdims=False)
            return [pieces[k] for k in range(CHUNKS)]

        def collect(slabs):
            rows = gathered(jnp.stack(slabs), "gz", 1).reshape(tokens, slab)
            wide = lax.all_to_all(rows, "gy", split_axis=0, concat_axis=1, tiled=True)
            piece = wide.shape[1] // size_gz
            return lax.dynamic_slice_in_dim(wide, index_gz * piece, piece, 1)

    def sum_of(choices):
        chosen = choices[0][1]
        for condition, value in choices[1:]:
            chosen = jnp.where(condition, value, chosen)
        return chosen

    entering = [piece for m in range(micro_count) for piece in spread(micro_inputs[m])]

    gain_slab = lax.dynamic_slice_in_dim(norm_gain[0], index_gy * slab, slab, 0)[None, :]
    own_bias = jnp.concatenate(
        [
            lax.dynamic_slice_in_dim(q_bias[0], me * own_cols, own_cols, 0),
            lax.dynamic_slice_in_dim(kv_bias[0, 0], kv_start(me), used_cols, 0),
            lax.dynamic_slice_in_dim(kv_bias[0, 1], kv_start(me), used_cols, 0),
        ]
    )[None, :]

    order = (index_gz + jnp.arange(size_gz)) % size_gz
    row_pos = (order[:, None] * share + jnp.arange(share)[None, :]).reshape(chunk)
    half_width = HD // 2
    frequency = ROPE_BASE ** (-jnp.arange(half_width, dtype=jnp.float32) * 2.0 / HD)
    ticks = jobs + sections - 1
    ordinals = (jnp.arange(ticks) - index_section) % CHUNKS
    positions = ordinals[:, None] * chunk + row_pos[None, :]
    angles = positions.astype(jnp.float32)[:, :, None] * frequency[None, None, :]
    cosines = jnp.cos(angles)
    sines = jnp.sin(angles)
    cosines = list(jnp.concatenate([cosines, cosines], axis=-1))
    sines = list(jnp.concatenate([-sines, sines], axis=-1))
    causal = row_pos[None, :] <= row_pos[:, None]
    masks = [
        jnp.concatenate(
            [causal] + [jnp.broadcast_to(ordinals[t] >= j, (chunk, chunk)) for j in range(1, min(CHUNKS, t + 1))],
            axis=1,
        ).astype(jnp.float32)
        for t in range(ticks)
    ]
    conditions = [index_section == s for s in range(sections)]
    if even:
        conditions += [lax.rem(index_gz + j, size_gy) == k for j in range(CHUNKS) for k in range(CHUNKS)]
        conditions += [lax.rem(index_gy + size_gy - j, size_gz) == d for d in range(size_gz) for j in range(CHUNKS)]
    flags = jnp.broadcast_to(jnp.stack(conditions).astype(jnp.float32)[:, None], (len(conditions), 128))
    far_first = offsets[::-1]
    targets = [chip_at(dx, dy) for dx, dy in far_first]
    sources = [chip_at(size_gx - dx if dx else 0, size_gy - dy if dy else 0) for dx, dy in offsets]
    table = jnp.stack(targets + sources + [me]).astype(jnp.int32)
    mine = 2 * len(offsets)
    copies = []
    everything = slice(None)
    for chip in range(group):
        kv_from = chip * own_heads // group_size * HD
        target = (everything, pl.ds(chip * width, own_cols))
        copies.append((0, (0, everything, pl.ds(chip * own_cols, own_cols)), 0, target))
        for i in range(2):
            target = (everything, pl.ds(chip * width + own_cols + i * used_cols, used_cols))
            copies.append((1, (0, i, everything, pl.ds(kv_from, used_cols)), 0, target))
    kept = min(HELD_BLOCKS, len(offsets))
    held_copies = []
    for i in range(kept):
        slot = mine - 1 - i

        def where(table_ref, slot=slot):
            return 0, pl.ds(pl.multiple_of(table_ref[slot] * own_cols, 128), own_cols)

        held_copies.append((0, where, i, (everything,)))
    early = [gain_slab, own_bias, *cosines, *sines, *masks]
    table, flags, weights = resident([table, flags], early, [q_weight, kv_weight], copies, [(slab, group * width)])
    _, *held = resident([table], [], [out_weight], held_copies, [(own_cols, slab)] * kept)
    held = {mine - 1 - i: w for i, w in enumerate(held)}
    mixing_weight = pltpu.with_memory_space_constraint(out_weight, pltpu.HBM)

    def flag(i):
        return flags[i : i + 1, :1] > 0.5

    def layer(own_rows, tick, earlier):
        pieces = [own_rows] + [around(own_rows, "gz", -j) for j in range(1, size_gz)]
        scaled, total, part = enter(table, 0, pieces, gain_slab, weights, width)
        received = []
        for k, o in enumerate(far_first):
            if k:
                part = project_block(table, k, scaled, weights, width, jnp.bfloat16)
            received.append(to_offset(part, *o))
        totals = [total]
        for o in far_first:
            totals.append(to_offset(total, *o))
        projected = project_block(table, mine, scaled, weights, width, jnp.float32)
        attended, keys, values = attend(
            projected,
            received,
            totals,
            own_bias,
            cosines[tick],
            sines[tick],
            masks[tick],
            earlier[: CHUNKS - 1],
            own_heads,
            used_heads,
            features,
        )
        seen = [(keys, values)] + earlier
        arrived = []
        for o in offsets:
            arrived.append(to_offset(attended, *o))
        (sums,) = mix_blocks(table, [mine], [attended], mixing_weight, held, None, 1)
        back = list(range(len(offsets), mine))
        if len(offsets) > 1:
            (sums,) = mix_blocks(table, back[:-1], arrived[:-1], mixing_weight, held, sums, 1)
        own_sum, *others = mix_blocks(table, back[-1:], arrived[-1:], mixing_weight, held, sums, size_gz)
        result = leave(own_rows, own_sum, [around(piece, "gz", j + 1) for j, piece in enumerate(others)])
        return result, seen

    results = []
    carried = None
    earlier = []
    for tick in range(ticks):
        if carried is None:
            current = entering[0]
        elif tick < jobs:
            current = jnp.where(flag(0), entering[tick], carried)
        else:
            current = carried
        result, earlier = layer(current, tick, earlier)
        results.append(result)
        if tick < ticks - 1:
            carried = lax.ppermute(result, "section", [(i, i + 1) for i in range(sections - 1)])

    stored = [sum_of([(flag(s), results[job + s]) for s in range(sections)]) for job in range(jobs)]
    return jnp.stack([collect(stored[m * CHUNKS : (m + 1) * CHUNKS]) for m in range(micro_count)])[None]


def solution(mesh):
    return jax.shard_map(
        body,
        mesh=mesh,
        in_specs=(
            P(None, "gy", ("gx", "gz")),
            P("section", "gx"),
            P("section", ("gx", "gy"), "gz"),
            P("section", None, ("gx", "gy"), "gz"),
            P("section", "gz"),
            P("section", None, "gz"),
            P("section", "gz", ("gx", "gy")),
        ),
        out_specs=P("section", None, "gy", ("gx", "gz")),
        check_vma=False,
    )
```

```python
import jax
import jax.numpy as jnp
from jax import lax
from jax.experimental import pallas as pl
from jax.experimental.pallas import tpu as pltpu
from jax.sharding import PartitionSpec as P

HD = 128
ROPE_BASE = 1000000.0
EPSILON = 1e-06
NEG_FILL = -1e30
CHUNKS = 2
TAIL = 8
HELD_BLOCKS = 3
WHOLE = pl.BlockSpec(memory_space=pltpu.VMEM)
SCALARS = pl.BlockSpec(memory_space=pltpu.SMEM)
LIMIT = pltpu.CompilerParams(vmem_limit_bytes=4 << 20)


def tile_of(columns):
    return 256 if columns % 256 == 0 else 128


def effort(flops, moved=0):
    return pl.CostEstimate(flops=flops, transcendentals=0, bytes_accessed=moved)


def resident(small, early, sources, copies, shapes):
    def kernel(*refs):
        small_refs = refs[: len(small)]
        source_refs = refs[len(small) : len(small) + len(sources)]
        outs = refs[len(small) + len(sources) + len(early) :]
        moves = []
        for i, (source, where, held, target) in enumerate(copies):
            where = where(small_refs[0]) if callable(where) else where
            moves.append(
                pltpu.make_async_copy(source_refs[source].at[where], outs[len(small) + held].at[target], outs[-1].at[i])
            )
        for move in moves:
            move.start()
        for value, ref, out in zip(small, small_refs, outs):
            if value.dtype == jnp.int32:
                for i in range(value.shape[0]):
                    out[i] = ref[i]
            else:
                out[...] = ref[...]
        for move in moves:
            move.wait()

    def space(value):
        return SCALARS if value.dtype == jnp.int32 else WHOLE

    return pl.pallas_call(
        kernel,
        out_shape=[(pltpu.SMEM if v.dtype == jnp.int32 else pltpu.VMEM)(v.shape, v.dtype) for v in small]
        + [pltpu.VMEM(shape, jnp.bfloat16) for shape in shapes],
        in_specs=[space(v) for v in small] + [pl.BlockSpec(memory_space=pltpu.HBM)] * len(sources)
        + [pl.BlockSpec(memory_space=pl.ANY)] * len(early),
        out_specs=[space(v) for v in small] + [WHOLE] * len(shapes),
        scratch_shapes=[pltpu.SemaphoreType.DMA((len(copies),))],
        compiler_params=pltpu.CompilerParams(vmem_limit_bytes=1 << 20),
        cost_estimate=effort(1 << 32),
    )(*small, *[pltpu.with_memory_space_constraint(x, pltpu.HBM) for x in sources], *early)


def project_into(refs, x_ref, w_ref, start, width):
    tile = tile_of(width)
    rows = x_ref.shape[0] // len(refs)

    def step(i, _):
        spot = pl.ds(pl.multiple_of(i * tile, 128), tile)
        out = jnp.dot(
            x_ref[...],
            w_ref[:, pl.ds(pl.multiple_of(start + i * tile, 128), tile)],
            preferred_element_type=jnp.float32,
        )
        for h, ref in enumerate(refs):
            ref[:rows, spot] = out[h * rows : (h + 1) * rows].astype(ref.dtype)
        return 0

    lax.fori_loop(0, width // tile, step, 0)


def project_block(table, slot, rows, weight, width, kind, pieces=1):
    def kernel(table_ref, x_ref, w_ref, *refs):
        project_into(refs, x_ref, w_ref, table_ref[slot] * width, width)

    return pl.pallas_call(
        kernel,
        out_shape=[jax.ShapeDtypeStruct((rows.shape[0] // pieces, width), kind)] * pieces,
        in_specs=[SCALARS, WHOLE, WHOLE],
        out_specs=[WHOLE] * pieces,
        compiler_params=LIMIT,
        cost_estimate=effort(2 * rows.shape[0] * rows.shape[1] * width),
    )(table, rows, weight)


def write_split(ref, start, row):
    upper = row.astype(jnp.bfloat16)
    rest = row - upper.astype(jnp.float32)
    middle = rest.astype(jnp.bfloat16)
    lower = (rest - middle.astype(jnp.float32)).astype(jnp.bfloat16)
    zero = jnp.zeros((TAIL - 3, row.shape[1]), jnp.bfloat16)
    ref[start:, : row.shape[1]] = jnp.concatenate([upper, middle, lower, zero], axis=0)
    if ref.shape[1] > row.shape[1]:
        ref[start:, row.shape[1] :] = jnp.zeros((TAIL, ref.shape[1] - row.shape[1]), jnp.bfloat16)


def read_split(ref, start, size):
    value = ref[start : start + TAIL, :size].astype(jnp.float32)
    return value[0:1] + value[1:2] + value[2:3]


def enter(table, slot, pieces, gain, weight, width, halves):
    count = len(pieces)
    share, slab = pieces[0].shape
    chunk = share * count
    half = chunk // halves
    tail = TAIL if halves > 1 else 0

    def kernel(table_ref, gain_ref, w_ref, *refs):
        scaled_ref, total_ref, *o_refs = refs[count:]
        totals = []
        for i in range(count):
            wide = refs[i][...].astype(jnp.float32)
            scaled_ref[i * share : (i + 1) * share, :] = (wide * gain_ref[...]).astype(jnp.bfloat16)
            totals.append(jnp.sum(wide * wide, axis=1, keepdims=True))
        total = jnp.broadcast_to(jnp.concatenate(totals, axis=0), (chunk, 128))
        total = jnp.transpose(total)[:8]
        total_ref[...] = total
        if tail:
            write_split(o_refs[0], half, total[0:1])
        project_into(o_refs, scaled_ref, w_ref, table_ref[slot] * width, width)

    return pl.pallas_call(
        kernel,
        out_shape=[
            jax.ShapeDtypeStruct((chunk, slab), jnp.bfloat16),
            jax.ShapeDtypeStruct((8, chunk), jnp.float32),
        ]
        + [jax.ShapeDtypeStruct((half + (tail if h == 0 else 0), width), jnp.bfloat16) for h in range(halves)],
        in_specs=[SCALARS] + [WHOLE] * (2 + count),
        out_specs=[WHOLE] * (2 + halves),
        compiler_params=LIMIT,
        cost_estimate=effort(2 * chunk * slab * width),
    )(table, gain, weight, *pieces)


def attend(projected, received, totals, bias, cosine, sine, mask, earlier, heads, used, features):
    chunk = projected.shape[0]
    halves = len(received)
    half = chunk // halves
    counts = [len(parts) for parts in received]
    group = heads // used
    own_cols = heads * HD
    used_cols = used * HD
    parts = sum(counts)
    summed = len(totals)
    past = len(earlier)
    scale = HD ** (-0.5)

    def kernel(p_ref, bias_ref, cos_ref, sin_ref, mask_ref, *refs):
        part_refs = [refs[sum(counts[:h]) : sum(counts[: h + 1])] for h in range(halves)]
        total_refs = refs[parts : parts + summed]
        past_refs = refs[parts + summed : parts + summed + 2 * past]
        *o_refs, k_ref, v_ref = refs[parts + summed + 2 * past :]
        total = total_refs[0][0:1, :]
        for ref in total_refs[1:]:
            total = total + ref[0:1, :]
        for ref in [r for parts_of in part_refs for r in parts_of if r.shape[0] > half]:
            total = total + read_split(ref, half, chunk)
        inverse = lax.rsqrt(total / features + EPSILON)
        inverse = jnp.transpose(jnp.broadcast_to(inverse, (HD, chunk)))
        cosine_rows = cos_ref[...]
        sine_rows = sin_ref[...]

        def columns(start):
            pieces = []
            for h in range(halves):
                piece = p_ref[h * half : (h + 1) * half, start : start + HD]
                for ref in part_refs[h]:
                    piece = piece + ref[:half, start : start + HD].astype(jnp.float32)
                pieces.append(piece)
            value = jnp.concatenate(pieces, axis=0) if halves > 1 else pieces[0]
            return value * inverse + bias_ref[:, start : start + HD]

        def rotate(value):
            return (value * cosine_rows + pltpu.roll(value, HD // 2, 1) * sine_rows).astype(jnp.bfloat16)

        allowed = mask_ref[...] > 0.5
        for u in range(used):
            spot = slice(u * HD, (u + 1) * HD)
            k_ref[:, spot] = rotate(columns(own_cols + u * HD))
            v_ref[:, spot] = columns(own_cols + used_cols + u * HD).astype(jnp.bfloat16)
            keys = [k_ref[:, spot]] + [past_refs[2 * j][:, spot] for j in range(past)]
            values = [v_ref[:, spot]] + [past_refs[2 * j + 1][:, spot] for j in range(past)]
            keys = jnp.concatenate(keys, axis=0) if past else keys[0]
            values = jnp.concatenate(values, axis=0) if past else values[0]
            for g in range(group):
                start = (u * group + g) * HD
                query = rotate(columns(start))
                scores = (
                    lax.dot_general(query, keys, (((1,), (1,)), ((), ())), preferred_element_type=jnp.float32) * scale
                )
                scores = jnp.where(allowed, scores, NEG_FILL)
                weights = jnp.where(allowed, jnp.exp(scores - jnp.max(scores, axis=1, keepdims=True)), 0.0)
                denominator = jnp.sum(weights, axis=1, keepdims=True)
                mixed = jnp.dot(weights.astype(jnp.bfloat16), values, preferred_element_type=jnp.float32)
                attended = (mixed / denominator).astype(jnp.bfloat16)
                for h, o_ref in enumerate(o_refs):
                    o_ref[:, start : start + HD] = attended[h * half : (h + 1) * half]

    return pl.pallas_call(
        kernel,
        out_shape=[jax.ShapeDtypeStruct((half, own_cols), jnp.bfloat16)] * halves
        + [jax.ShapeDtypeStruct((chunk, used_cols), jnp.bfloat16)] * 2,
        in_specs=[WHOLE] * (5 + parts + summed + 2 * past),
        out_specs=[WHOLE] * (halves + 2),
        compiler_params=LIMIT,
        cost_estimate=effort(1 << 29),
    )(projected, bias, cosine, sine, mask, *[p for parts in received for p in parts], *totals, *[a for pair in earlier for a in pair])


def mix_blocks(table, slots, blocks, weight, held, so_far, cores):
    count = len(blocks)
    pieces = len(blocks[0])
    depth = blocks[0][0].shape[1]
    chunk = blocks[0][0].shape[0] * pieces
    slab = weight.shape[2]
    share = chunk // cores
    tile = min(slab, 512)
    near = [b for b in range(count) if slots[b] in held]
    steps = [(i, b) for i in range(slab // tile) for b in range(count) if b not in near]
    buffers = min(4, len(steps))
    ready = [held[slots[b]] for b in near]
    inputs = [*ready, *[p for block in blocks for p in block]] + ([] if so_far is None else [so_far])

    def kernel(table_ref, w_ref, *refs):
        outs = refs[len(inputs) : len(inputs) + cores]
        rows_of = [refs[len(ready) + b * pieces : len(ready) + (b + 1) * pieces] for b in range(count)]
        fetches = []
        for step, (i, b) in enumerate(steps):
            row = pl.multiple_of(table_ref[slots[b]] * depth, 128)
            buffer, sems = refs[-2:]
            fetches.append(
                pltpu.make_async_copy(
                    w_ref.at[0, pl.ds(row, depth), pl.ds(i * tile, tile)],
                    buffer.at[step % buffers],
                    sems.at[step % buffers],
                )
            )
        for fetch in fetches[:buffers]:
            fetch.start()
        left = [jnp.concatenate([r[...] for r in p], axis=0) if pieces > 1 else p[0][...] for p in rows_of]
        for i in range(slab // tile):
            spot = slice(i * tile, (i + 1) * tile)
            out = None if so_far is None else refs[len(inputs) - 1][:, spot]
            for b in near + [b for b in range(count) if b not in near]:
                if b in near:
                    rows = refs[near.index(b)][:, spot]
                else:
                    step = steps.index((i, b))
                    fetches[step].wait()
                    rows = refs[-2][step % buffers]
                term = jnp.dot(left[b], rows, preferred_element_type=jnp.float32)
                out = term if out is None else out + term
                if b not in near and step + buffers < len(steps):
                    fetches[step + buffers].start()
            for j, ref in enumerate(outs):
                ref[:, spot] = out[j * share : (j + 1) * share].astype(ref.dtype)

    scratch = [pltpu.VMEM((buffers, depth, tile), jnp.bfloat16), pltpu.SemaphoreType.DMA((buffers,))]
    return pl.pallas_call(
        kernel,
        out_shape=[
            jax.ShapeDtypeStruct((share, slab), jnp.bfloat16 if j else jnp.float32) for j in range(cores)
        ],
        in_specs=[SCALARS, pl.BlockSpec(memory_space=pltpu.HBM)] + [WHOLE] * len(inputs),
        out_specs=[WHOLE] * cores,
        scratch_shapes=scratch if steps else [],
        compiler_params=pltpu.CompilerParams(vmem_limit_bytes=8 << 20),
        cost_estimate=effort(2 * count * chunk * depth * slab),
    )(table, weight, *inputs)


def fold(part_x, part_y, from_x, from_y, total):
    half, _ = part_x.shape
    chunk = total.shape[1]

    def kernel(x_ref, y_ref, from_x_ref, from_y_ref, total_ref, to_y_ref, to_x_ref, pair_ref):
        to_y_ref[:half] = (y_ref[...].astype(jnp.float32) + from_x_ref[:half].astype(jnp.float32)).astype(jnp.bfloat16)
        to_x_ref[...] = (x_ref[...].astype(jnp.float32) + from_y_ref[...].astype(jnp.float32)).astype(jnp.bfloat16)
        pair = total_ref[0:1, :] + read_split(from_x_ref, half, chunk)
        write_split(to_y_ref, half, pair)
        pair_ref[...] = jnp.broadcast_to(pair, (8, chunk))

    return pl.pallas_call(
        kernel,
        out_shape=[
            jax.ShapeDtypeStruct(from_x.shape, jnp.bfloat16),
            jax.ShapeDtypeStruct(from_y.shape, jnp.bfloat16),
            jax.ShapeDtypeStruct(total.shape, jnp.float32),
        ],
        in_specs=[WHOLE] * 5,
        out_specs=[WHOLE] * 3,
        compiler_params=LIMIT,
        cost_estimate=effort(1 << 26),
    )(part_x, part_y, from_x, from_y, total)


def pick(table, slots, choices, joined=False):
    shape = choices[0].shape
    count = len(slots)

    def kernel(table_ref, *refs):
        for i, slot in enumerate(slots):
            for k in range(len(choices)):

                @pl.when(table_ref[slot] == k)
                def _():
                    if joined:
                        refs[-1][i * shape[0] : (i + 1) * shape[0]] = refs[k][...]
                    else:
                        refs[len(choices) + i][...] = refs[k][...]

    if joined:
        outs = [jax.ShapeDtypeStruct((count * shape[0], shape[1]), choices[0].dtype)]
    else:
        outs = [jax.ShapeDtypeStruct(shape, choices[0].dtype)] * count
    return pl.pallas_call(
        kernel,
        out_shape=outs,
        in_specs=[SCALARS] + [WHOLE] * len(choices),
        out_specs=[WHOLE] * len(outs),
        compiler_params=LIMIT,
        cost_estimate=effort(1 << 24),
    )(table, *choices)


def leave(rows, own_sum, pieces):
    def kernel(x_ref, sum_ref, *refs):
        value = x_ref[...].astype(jnp.float32) + sum_ref[...]
        for ref in refs[:-1]:
            value = value + ref[...].astype(jnp.float32)
        refs[-1][...] = value.astype(jnp.bfloat16)

    return pl.pallas_call(
        kernel,
        out_shape=jax.ShapeDtypeStruct(rows.shape, jnp.bfloat16),
        in_specs=[WHOLE] * (2 + len(pieces)),
        out_specs=WHOLE,
        compiler_params=LIMIT,
        cost_estimate=effort(1 << 26),
    )(rows, own_sum, *pieces)


def around(value, axis, steps):
    count = lax.axis_size(axis)
    return lax.ppermute(value, axis, [(i, (i + steps) % count) for i in range(count)])


def gathered(value, axis, dim):
    pieces = [value] + [around(value, axis, -j) for j in range(1, lax.axis_size(axis))]
    count = lax.axis_size(axis)
    stacked = jnp.take(jnp.stack(pieces), (jnp.arange(count) - lax.axis_index(axis)) % count, axis=0)
    shape = list(value.shape)
    shape[dim] *= count
    return jnp.moveaxis(stacked, 0, dim).reshape(shape)


def body(micro_inputs, norm_gain, q_weight, kv_weight, q_bias, kv_bias, out_weight):
    sections = lax.axis_size("section")
    size_gx, size_gy, size_gz = (lax.axis_size(a) for a in ("gx", "gy", "gz"))
    group = size_gx * size_gy
    index_gx, index_gy, index_gz = (lax.axis_index(a) for a in ("gx", "gy", "gz"))
    index_section = lax.axis_index("section")
    me = index_gx * size_gy + index_gy
    micro_count = micro_inputs.shape[0]
    tokens = micro_inputs.shape[1] * size_gy
    features = micro_inputs.shape[2] * size_gx * size_gz
    slab = q_weight.shape[1]
    chunk = tokens // CHUNKS
    share = chunk // size_gz
    q_cols = q_weight.shape[2]
    kv_cols = kv_weight.shape[3]
    group_size = q_cols // kv_cols
    own_cols = q_cols // group
    own_heads = own_cols // HD
    used_heads = max(1, own_heads // group_size)
    used_cols = used_heads * HD
    width = own_cols + 2 * used_cols
    jobs = micro_count * CHUNKS

    offsets = [(dx, dy) for dx in range(size_gx) for dy in range(size_gy)][1:]
    offsets.sort(key=lambda o: (min(o[0], size_gx - o[0]) + min(o[1], size_gy - o[1])))

    def chip_at(dx, dy):
        x = index_gx + dx
        y = index_gy + dy
        return jnp.where(x >= size_gx, x - size_gx, x) * size_gy + jnp.where(y >= size_gy, y - size_gy, y)

    def to_offset(value, dx, dy):
        pairs = [
            (x * size_gy + y, (x + dx) % size_gx * size_gy + (y + dy) % size_gy)
            for x in range(size_gx)
            for y in range(size_gy)
        ]
        return lax.ppermute(value, ("gx", "gy"), pairs)

    def kv_start(chip):
        return chip * own_heads // group_size * HD

    even = size_gy == size_gz == CHUNKS
    if even:

        def spread(block):
            cut = block.reshape(size_gz, share, slab)
            pieces = []
            for j in range(CHUNKS):
                spot = lax.rem(index_gy + j, size_gz)
                pairs = [
                    (a * size_gz + b, b * size_gz + (a + j) % size_gz) for a in range(size_gy) for b in range(size_gz)
                ]
                piece = lax.dynamic_index_in_dim(cut, spot, 0, keepdims=False)
                pieces.append(lax.ppermute(piece, ("gy", "gz"), pairs))
            return [
                sum_of([(lax.rem(index_gz + size_gz - j, size_gz) == k, pieces[j]) for j in range(CHUNKS)])
                for k in range(CHUNKS)
            ]

        def collect(found):
            sent = pick(table, range(picks, picks + CHUNKS), found)
            pieces = []
            for j in range(CHUNKS):
                pairs = [
                    (c * size_gz + d, (d + j) % size_gy * size_gz + c) for c in range(size_gy) for d in range(size_gz)
                ]
                pieces.append(lax.ppermute(sent[j], ("gy", "gz"), pairs))
            (rows,) = pick(table, range(picks + CHUNKS, picks + CHUNKS + size_gz), pieces, joined=True)
            return rows
    else:

        def spread(block):
            wide = gathered(block, "gz", 1)
            pieces = lax.all_to_all(wide, "gy", split_axis=1, concat_axis=0, tiled=True)
            pieces = pieces.reshape(CHUNKS, size_gz, share, slab)
            pieces = lax.dynamic_index_in_dim(pieces, index_gz, 1, keepdims=False)
            return [pieces[k] for k in range(CHUNKS)]

        def collect(found):
            slabs = [pick(table, [mine + 1], found[k : k + sections])[0] for k in range(CHUNKS)]
            rows = gathered(jnp.stack(slabs), "gz", 1).reshape(tokens, slab)
            wide = lax.all_to_all(rows, "gy", split_axis=0, concat_axis=1, tiled=True)
            piece = wide.shape[1] // size_gz
            return lax.dynamic_slice_in_dim(wide, index_gz * piece, piece, 1)

    def sum_of(choices):
        chosen = choices[0][1]
        for condition, value in choices[1:]:
            chosen = jnp.where(condition, value, chosen)
        return chosen

    gain_slab = lax.dynamic_slice_in_dim(norm_gain[0], index_gy * slab, slab, 0)[None, :]
    own_bias = jnp.concatenate(
        [
            lax.dynamic_slice_in_dim(q_bias[0], me * own_cols, own_cols, 0),
            lax.dynamic_slice_in_dim(kv_bias[0, 0], kv_start(me), used_cols, 0),
            lax.dynamic_slice_in_dim(kv_bias[0, 1], kv_start(me), used_cols, 0),
        ]
    )[None, :]

    order = (index_gz + jnp.arange(size_gz)) % size_gz
    row_pos = (order[:, None] * share + jnp.arange(share)[None, :]).reshape(chunk)
    half_width = HD // 2
    frequency = ROPE_BASE ** (-jnp.arange(half_width, dtype=jnp.float32) * 2.0 / HD)
    ticks = jobs + sections - 1
    ordinals = (jnp.arange(ticks) - index_section) % CHUNKS
    positions = ordinals[:, None] * chunk + row_pos[None, :]
    angles = positions.astype(jnp.float32)[:, :, None] * frequency[None, None, :]
    cosines = jnp.cos(angles)
    sines = jnp.sin(angles)
    cosines = list(jnp.concatenate([cosines, cosines], axis=-1))
    sines = list(jnp.concatenate([-sines, sines], axis=-1))
    causal = row_pos[None, :] <= row_pos[:, None]
    masks = [
        jnp.concatenate(
            [causal] + [jnp.broadcast_to(ordinals[t] >= j, (chunk, chunk)) for j in range(1, min(CHUNKS, t + 1))],
            axis=1,
        ).astype(jnp.float32)
        for t in range(ticks)
    ]
    far_first = offsets[::-1]
    square = size_gx == size_gy == 2
    targets = [chip_at(dx, dy) for dx, dy in far_first]
    sources = [chip_at(size_gx - dx if dx else 0, size_gy - dy if dy else 0) for dx, dy in offsets]
    mine = 2 * len(offsets)
    choice = [index_section, jnp.minimum(index_section, 1)]
    picks = mine + 1 + len(choice)
    if even:
        choice += [lax.rem(index_gz + j, size_gy) + index_section for j in range(CHUNKS)]
        choice += [lax.rem(index_gy + size_gy - d, size_gz) for d in range(size_gz)]
    table = jnp.stack(targets + sources + [me] + choice).astype(jnp.int32)
    early = [gain_slab, own_bias, *cosines, *sines, *masks]
    (table, early, micro_inputs) = lax.optimization_barrier((table, early, micro_inputs))
    gain_slab, own_bias = early[:2]
    cosines, sines, masks = (early[2 + i * ticks : 2 + (i + 1) * ticks] for i in range(3))
    entering = [piece for m in range(micro_count) for piece in spread(micro_inputs[m])]

    copies = []
    everything = slice(None)
    for chip in range(group):
        kv_from = chip * own_heads // group_size * HD
        target = (everything, pl.ds(chip * width, own_cols))
        copies.append((0, (0, everything, pl.ds(chip * own_cols, own_cols)), 0, target))
        for i in range(2):
            target = (everything, pl.ds(chip * width + own_cols + i * used_cols, used_cols))
            copies.append((1, (0, i, everything, pl.ds(kv_from, used_cols)), 0, target))
    kept = min(HELD_BLOCKS, len(offsets))
    held_copies = []
    for i in range(kept):
        slot = mine - 1 - i

        def where(table_ref, slot=slot):
            return 0, pl.ds(pl.multiple_of(table_ref[slot] * own_cols, 128), own_cols)

        held_copies.append((0, where, i, (everything,)))
    table, weights = resident([table], early, [q_weight, kv_weight], copies, [(slab, group * width)])
    _, *held = resident([table], [], [out_weight], held_copies, [(own_cols, slab)] * kept)
    held = {mine - 1 - i: w for i, w in enumerate(held)}
    mixing_weight = pltpu.with_memory_space_constraint(out_weight, pltpu.HBM)

    def layer(own_rows, tick, earlier):
        pieces = [own_rows] + [around(own_rows, "gz", -j) for j in range(1, size_gz)]
        scaled, total, *part = enter(table, 0, pieces, gain_slab, weights, width, 2 if square else 1)
        if square:
            from_x = to_offset(part[0], 1, 0)
            from_y = to_offset(part[1], 0, 1)
            later_y, near_y = project_block(table, 2, scaled, weights, width, jnp.bfloat16, 2)
            direct_y = to_offset(near_y, 0, 1)
            near_x, later_x = project_block(table, 1, scaled, weights, width, jnp.bfloat16, 2)
            direct_x = to_offset(near_x, 1, 0)
            to_y, to_x, total = fold(later_x, later_y, from_x, from_y, total)
            folded_y = to_offset(to_y, 0, 1)
            folded_x = to_offset(to_x, 1, 0)
            received = [[direct_x, folded_y], [direct_y, folded_x]]
            totals = [total]
        else:
            received = [[]]
            totals = [total]
            part = part[0]
            for k, o in enumerate(far_first):
                if k:
                    (part,) = project_block(table, k, scaled, weights, width, jnp.bfloat16)
                received[0].append(to_offset(part, *o))
            for o in far_first:
                totals.append(to_offset(total, *o))
        (projected,) = project_block(table, mine, scaled, weights, width, jnp.float32)
        *attended, keys, values = attend(
            projected,
            received,
            totals,
            own_bias,
            cosines[tick],
            sines[tick],
            masks[tick],
            earlier[: CHUNKS - 1],
            own_heads,
            used_heads,
            features,
        )
        seen = [(keys, values)] + earlier
        arrived = []
        if square:
            x_upper = to_offset(attended[0], 1, 0)
            y_lower = to_offset(attended[1], 0, 1)
            x_lower = to_offset(attended[1], 1, 0)
            y_upper = to_offset(attended[0], 0, 1)
            far_upper = to_offset(x_upper, 0, 1)
            far_lower = to_offset(y_lower, 1, 0)
            arrived = [(y_upper, y_lower), (x_upper, x_lower), (far_upper, far_lower)]
        else:
            for o in offsets:
                arrived.append((to_offset(attended[0], *o),))
        (sums,) = mix_blocks(table, [mine], [tuple(attended)], mixing_weight, held, None, 1)
        back = list(range(len(offsets), mine))
        if len(offsets) > 1:
            (sums,) = mix_blocks(table, back[:-1], arrived[:-1], mixing_weight, held, sums, 1)
        own_sum, *others = mix_blocks(table, back[-1:], arrived[-1:], mixing_weight, held, sums, size_gz)
        result = leave(own_rows, own_sum, [around(piece, "gz", j + 1) for j, piece in enumerate(others)])
        return result, seen

    results = []
    carried = None
    earlier = []
    for tick in range(ticks):
        if carried is None:
            current = entering[0]
        elif tick < jobs:
            (current,) = pick(table, [mine + 2], [entering[tick], carried])
        else:
            current = carried
        result, earlier = layer(current, tick, earlier)
        results.append(result)
        if tick < ticks - 1:
            carried = lax.ppermute(result, "section", [(i, i + 1) for i in range(sections - 1)])

    cuts = [results[m * CHUNKS : (m + 1) * CHUNKS + sections - 1] for m in range(micro_count)]
    return jnp.stack([collect(found) for found in cuts])[None]


def solution(mesh):
    return jax.shard_map(
        body,
        mesh=mesh,
        in_specs=(
            P(None, "gy", ("gx", "gz")),
            P("section", "gx"),
            P("section", ("gx", "gy"), "gz"),
            P("section", None, ("gx", "gy"), "gz"),
            P("section", "gz"),
            P("section", None, "gz"),
            P("section", "gz", ("gx", "gy")),
        ),
        out_specs=P("section", None, "gy", ("gx", "gz")),
        check_vma=False,
    )
```

```python
import jax
import jax.numpy as jnp
from jax import lax
from jax.experimental import pallas as pl
from jax.experimental.pallas import tpu as pltpu
from jax.sharding import PartitionSpec as P

HD = 128
ROPE_BASE = 1000000.0
EPSILON = 1e-06
NEG_FILL = -1e30
CHUNKS = 2
TAIL = 8
HELD_BLOCKS = 3
WHOLE = pl.BlockSpec(memory_space=pltpu.VMEM)
SCALARS = pl.BlockSpec(memory_space=pltpu.SMEM)
LIMIT = pltpu.CompilerParams(vmem_limit_bytes=4 << 20)


def tile_of(columns):
    return 256 if columns % 256 == 0 else 128


def effort(flops, moved=0):
    return pl.CostEstimate(flops=flops, transcendentals=0, bytes_accessed=moved)


def resident(small, early, sources, copies, shapes):
    def kernel(*refs):
        small_refs = refs[: len(small)]
        source_refs = refs[len(small) : len(small) + len(sources)]
        outs = refs[len(small) + len(sources) + len(early) :]
        moves = []
        for i, (source, where, held, target) in enumerate(copies):
            where = where(small_refs[0]) if callable(where) else where
            moves.append(
                pltpu.make_async_copy(source_refs[source].at[where], outs[len(small) + held].at[target], outs[-1].at[i])
            )
        for move in moves:
            move.start()
        for value, ref, out in zip(small, small_refs, outs):
            if value.dtype == jnp.int32:
                for i in range(value.shape[0]):
                    out[i] = ref[i]
            else:
                out[...] = ref[...]
        for move in moves:
            move.wait()

    def space(value):
        return SCALARS if value.dtype == jnp.int32 else WHOLE

    return pl.pallas_call(
        kernel,
        out_shape=[(pltpu.SMEM if v.dtype == jnp.int32 else pltpu.VMEM)(v.shape, v.dtype) for v in small]
        + [pltpu.VMEM(shape, jnp.bfloat16) for shape in shapes],
        in_specs=[space(v) for v in small] + [pl.BlockSpec(memory_space=pltpu.HBM)] * len(sources)
        + [pl.BlockSpec(memory_space=pl.ANY)] * len(early),
        out_specs=[space(v) for v in small] + [WHOLE] * len(shapes),
        scratch_shapes=[pltpu.SemaphoreType.DMA((len(copies),))],
        compiler_params=pltpu.CompilerParams(vmem_limit_bytes=1 << 20),
        cost_estimate=effort(1 << 32),
    )(*small, *[pltpu.with_memory_space_constraint(x, pltpu.HBM) for x in sources], *early)


def project_into(refs, x_ref, w_ref, start, width):
    tile = tile_of(width)
    rows = x_ref.shape[0] // len(refs)

    def step(i, _):
        spot = pl.ds(pl.multiple_of(i * tile, 128), tile)
        out = jnp.dot(
            x_ref[...],
            w_ref[:, pl.ds(pl.multiple_of(start + i * tile, 128), tile)],
            preferred_element_type=jnp.float32,
        )
        for h, ref in enumerate(refs):
            ref[:rows, spot] = out[h * rows : (h + 1) * rows].astype(ref.dtype)
        return 0

    lax.fori_loop(0, width // tile, step, 0)


def project_block(table, slot, rows, weight, width, kind, pieces=1):
    def kernel(table_ref, x_ref, w_ref, *refs):
        project_into(refs, x_ref, w_ref, table_ref[slot] * width, width)

    return pl.pallas_call(
        kernel,
        out_shape=[jax.ShapeDtypeStruct((rows.shape[0] // pieces, width), kind)] * pieces,
        in_specs=[SCALARS, WHOLE, WHOLE],
        out_specs=[WHOLE] * pieces,
        compiler_params=LIMIT,
        cost_estimate=effort(2 * rows.shape[0] * rows.shape[1] * width),
    )(table, rows, weight)


def write_split(ref, start, row):
    upper = row.astype(jnp.bfloat16)
    rest = row - upper.astype(jnp.float32)
    middle = rest.astype(jnp.bfloat16)
    lower = (rest - middle.astype(jnp.float32)).astype(jnp.bfloat16)
    zero = jnp.zeros((TAIL - 3, row.shape[1]), jnp.bfloat16)
    ref[start:, : row.shape[1]] = jnp.concatenate([upper, middle, lower, zero], axis=0)
    if ref.shape[1] > row.shape[1]:
        ref[start:, row.shape[1] :] = jnp.zeros((TAIL, ref.shape[1] - row.shape[1]), jnp.bfloat16)


def read_split(ref, start, size):
    value = ref[start : start + TAIL, :size].astype(jnp.float32)
    return value[0:1] + value[1:2] + value[2:3]


def enter(table, slot, pieces, gain, weight, width, halves):
    count = len(pieces)
    share, slab = pieces[0].shape
    chunk = share * count
    half = chunk // halves
    tail = TAIL if halves > 1 else 0

    def kernel(table_ref, gain_ref, w_ref, *refs):
        scaled_ref, total_ref, *o_refs = refs[count:]
        totals = []
        for i in range(count):
            wide = refs[i][...].astype(jnp.float32)
            scaled_ref[i * share : (i + 1) * share, :] = (wide * gain_ref[...]).astype(jnp.bfloat16)
            totals.append(jnp.sum(wide * wide, axis=1, keepdims=True))
        total = jnp.broadcast_to(jnp.concatenate(totals, axis=0), (chunk, 128))
        total = jnp.transpose(total)[:8]
        total_ref[...] = total
        if tail:
            write_split(o_refs[0], half, total[0:1])
        project_into(o_refs, scaled_ref, w_ref, table_ref[slot] * width, width)

    return pl.pallas_call(
        kernel,
        out_shape=[
            jax.ShapeDtypeStruct((chunk, slab), jnp.bfloat16),
            jax.ShapeDtypeStruct((8, chunk), jnp.float32),
        ]
        + [jax.ShapeDtypeStruct((half + (tail if h == 0 else 0), width), jnp.bfloat16) for h in range(halves)],
        in_specs=[SCALARS] + [WHOLE] * (2 + count),
        out_specs=[WHOLE] * (2 + halves),
        compiler_params=LIMIT,
        cost_estimate=effort(2 * chunk * slab * width),
    )(table, gain, weight, *pieces)


def attend(projected, received, totals, bias, cosine, sine, mask, earlier, heads, used, features):
    chunk = projected.shape[0]
    halves = len(received)
    half = chunk // halves
    counts = [len(parts) for parts in received]
    group = heads // used
    own_cols = heads * HD
    used_cols = used * HD
    parts = sum(counts)
    summed = len(totals)
    past = len(earlier)
    scale = HD ** (-0.5)

    def kernel(p_ref, bias_ref, cos_ref, sin_ref, mask_ref, *refs):
        part_refs = [refs[sum(counts[:h]) : sum(counts[: h + 1])] for h in range(halves)]
        total_refs = refs[parts : parts + summed]
        past_refs = refs[parts + summed : parts + summed + 2 * past]
        *o_refs, k_ref, v_ref = refs[parts + summed + 2 * past :]
        total = total_refs[0][0:1, :]
        for ref in total_refs[1:]:
            total = total + ref[0:1, :]
        for ref in [r for parts_of in part_refs for r in parts_of if r.shape[0] > half]:
            total = total + read_split(ref, half, chunk)
        inverse = lax.rsqrt(total / features + EPSILON)
        inverse = jnp.transpose(jnp.broadcast_to(inverse, (HD, chunk)))
        cosine_rows = cos_ref[...]
        sine_rows = sin_ref[...]

        def columns(start):
            pieces = []
            for h in range(halves):
                piece = p_ref[h * half : (h + 1) * half, start : start + HD]
                for ref in part_refs[h]:
                    piece = piece + ref[:half, start : start + HD].astype(jnp.float32)
                pieces.append(piece)
            value = jnp.concatenate(pieces, axis=0) if halves > 1 else pieces[0]
            return value * inverse + bias_ref[:, start : start + HD]

        def rotate(value):
            return (value * cosine_rows + pltpu.roll(value, HD // 2, 1) * sine_rows).astype(jnp.bfloat16)

        allowed = mask_ref[...] > 0.5
        for u in range(used):
            spot = slice(u * HD, (u + 1) * HD)
            k_ref[:, spot] = rotate(columns(own_cols + u * HD))
            v_ref[:, spot] = columns(own_cols + used_cols + u * HD).astype(jnp.bfloat16)
            keys = [k_ref[:, spot]] + [past_refs[2 * j][:, spot] for j in range(past)]
            values = [v_ref[:, spot]] + [past_refs[2 * j + 1][:, spot] for j in range(past)]
            keys = jnp.concatenate(keys, axis=0) if past else keys[0]
            values = jnp.concatenate(values, axis=0) if past else values[0]
            for g in range(group):
                start = (u * group + g) * HD
                query = rotate(columns(start))
                scores = (
                    lax.dot_general(query, keys, (((1,), (1,)), ((), ())), preferred_element_type=jnp.float32) * scale
                )
                scores = jnp.where(allowed, scores, NEG_FILL)
                weights = jnp.where(allowed, jnp.exp(scores - jnp.max(scores, axis=1, keepdims=True)), 0.0)
                denominator = jnp.sum(weights, axis=1, keepdims=True)
                mixed = jnp.dot(weights.astype(jnp.bfloat16), values, preferred_element_type=jnp.float32)
                attended = (mixed / denominator).astype(jnp.bfloat16)
                for h, o_ref in enumerate(o_refs):
                    o_ref[:, start : start + HD] = attended[h * half : (h + 1) * half]

    return pl.pallas_call(
        kernel,
        out_shape=[jax.ShapeDtypeStruct((half, own_cols), jnp.bfloat16)] * halves
        + [jax.ShapeDtypeStruct((chunk, used_cols), jnp.bfloat16)] * 2,
        in_specs=[WHOLE] * (5 + parts + summed + 2 * past),
        out_specs=[WHOLE] * (halves + 2),
        compiler_params=LIMIT,
        cost_estimate=effort(1 << 29),
    )(projected, bias, cosine, sine, mask, *[p for parts in received for p in parts], *totals, *[a for pair in earlier for a in pair])


def mix_blocks(table, slots, blocks, weight, held, so_far, cores):
    count = len(blocks)
    pieces = len(blocks[0])
    depth = blocks[0][0].shape[1]
    chunk = blocks[0][0].shape[0] * pieces
    slab = weight.shape[2]
    share = chunk // cores
    tile = min(slab, 512)
    near = [b for b in range(count) if slots[b] in held]
    steps = [(i, b) for i in range(slab // tile) for b in range(count) if b not in near]
    buffers = min(4, len(steps))
    ready = [held[slots[b]] for b in near]
    inputs = [*ready, *[p for block in blocks for p in block]] + ([] if so_far is None else [so_far])

    def kernel(table_ref, w_ref, *refs):
        outs = refs[len(inputs) : len(inputs) + cores]
        rows_of = [refs[len(ready) + b * pieces : len(ready) + (b + 1) * pieces] for b in range(count)]
        fetches = []
        for step, (i, b) in enumerate(steps):
            row = pl.multiple_of(table_ref[slots[b]] * depth, 128)
            buffer, sems = refs[-2:]
            fetches.append(
                pltpu.make_async_copy(
                    w_ref.at[0, pl.ds(row, depth), pl.ds(i * tile, tile)],
                    buffer.at[step % buffers],
                    sems.at[step % buffers],
                )
            )
        for fetch in fetches[:buffers]:
            fetch.start()
        left = [jnp.concatenate([r[...] for r in p], axis=0) if pieces > 1 else p[0][...] for p in rows_of]
        for i in range(slab // tile):
            spot = slice(i * tile, (i + 1) * tile)
            out = None if so_far is None else refs[len(inputs) - 1][:, spot]
            for b in near + [b for b in range(count) if b not in near]:
                if b in near:
                    rows = refs[near.index(b)][:, spot]
                else:
                    step = steps.index((i, b))
                    fetches[step].wait()
                    rows = refs[-2][step % buffers]
                term = jnp.dot(left[b], rows, preferred_element_type=jnp.float32)
                out = term if out is None else out + term
                if b not in near and step + buffers < len(steps):
                    fetches[step + buffers].start()
            for j, ref in enumerate(outs):
                ref[:, spot] = out[j * share : (j + 1) * share].astype(ref.dtype)

    scratch = [pltpu.VMEM((buffers, depth, tile), jnp.bfloat16), pltpu.SemaphoreType.DMA((buffers,))]
    return pl.pallas_call(
        kernel,
        out_shape=[
            jax.ShapeDtypeStruct((share, slab), jnp.bfloat16 if j else jnp.float32) for j in range(cores)
        ],
        in_specs=[SCALARS, pl.BlockSpec(memory_space=pltpu.HBM)] + [WHOLE] * len(inputs),
        out_specs=[WHOLE] * cores,
        scratch_shapes=scratch if steps else [],
        compiler_params=pltpu.CompilerParams(vmem_limit_bytes=8 << 20),
        cost_estimate=effort(2 * count * chunk * depth * slab),
    )(table, weight, *inputs)


def fold(part_x, part_y, from_x, from_y, total):
    half, _ = part_x.shape
    chunk = total.shape[1]

    def kernel(x_ref, y_ref, from_x_ref, from_y_ref, total_ref, to_y_ref, to_x_ref, pair_ref):
        to_y_ref[:half] = (y_ref[...].astype(jnp.float32) + from_x_ref[:half].astype(jnp.float32)).astype(jnp.bfloat16)
        to_x_ref[...] = (x_ref[...].astype(jnp.float32) + from_y_ref[...].astype(jnp.float32)).astype(jnp.bfloat16)
        pair = total_ref[0:1, :] + read_split(from_x_ref, half, chunk)
        write_split(to_y_ref, half, pair)
        pair_ref[...] = jnp.broadcast_to(pair, (8, chunk))

    return pl.pallas_call(
        kernel,
        out_shape=[
            jax.ShapeDtypeStruct(from_x.shape, jnp.bfloat16),
            jax.ShapeDtypeStruct(from_y.shape, jnp.bfloat16),
            jax.ShapeDtypeStruct(total.shape, jnp.float32),
        ],
        in_specs=[WHOLE] * 5,
        out_specs=[WHOLE] * 3,
        compiler_params=LIMIT,
        cost_estimate=effort(1 << 26),
    )(part_x, part_y, from_x, from_y, total)


def pick(table, slots, choices, joined=False):
    shape = choices[0].shape
    count = len(slots)

    def kernel(table_ref, *refs):
        for i, slot in enumerate(slots):
            for k in range(len(choices)):

                @pl.when(table_ref[slot] == k)
                def _():
                    if joined:
                        refs[-1][i * shape[0] : (i + 1) * shape[0]] = refs[k][...]
                    else:
                        refs[len(choices) + i][...] = refs[k][...]

    if joined:
        outs = [jax.ShapeDtypeStruct((count * shape[0], shape[1]), choices[0].dtype)]
    else:
        outs = [jax.ShapeDtypeStruct(shape, choices[0].dtype)] * count
    return pl.pallas_call(
        kernel,
        out_shape=outs,
        in_specs=[SCALARS] + [WHOLE] * len(choices),
        out_specs=[WHOLE] * len(outs),
        compiler_params=LIMIT,
        cost_estimate=effort(1 << 24),
    )(table, *choices)


def leave(rows, own_sum, pieces):
    def kernel(x_ref, sum_ref, *refs):
        value = x_ref[...].astype(jnp.float32) + sum_ref[...]
        for ref in refs[:-1]:
            value = value + ref[...].astype(jnp.float32)
        refs[-1][...] = value.astype(jnp.bfloat16)

    return pl.pallas_call(
        kernel,
        out_shape=jax.ShapeDtypeStruct(rows.shape, jnp.bfloat16),
        in_specs=[WHOLE] * (2 + len(pieces)),
        out_specs=WHOLE,
        compiler_params=LIMIT,
        cost_estimate=effort(1 << 26),
    )(rows, own_sum, *pieces)


def around(value, axis, steps):
    count = lax.axis_size(axis)
    return lax.ppermute(value, axis, [(i, (i + steps) % count) for i in range(count)])


def gathered(value, axis, dim):
    pieces = [value] + [around(value, axis, -j) for j in range(1, lax.axis_size(axis))]
    count = lax.axis_size(axis)
    stacked = jnp.take(jnp.stack(pieces), (jnp.arange(count) - lax.axis_index(axis)) % count, axis=0)
    shape = list(value.shape)
    shape[dim] *= count
    return jnp.moveaxis(stacked, 0, dim).reshape(shape)


def body(micro_inputs, norm_gain, q_weight, kv_weight, q_bias, kv_bias, out_weight):
    sections = lax.axis_size("section")
    size_gx, size_gy, size_gz = (lax.axis_size(a) for a in ("gx", "gy", "gz"))
    group = size_gx * size_gy
    index_gx, index_gy, index_gz = (lax.axis_index(a) for a in ("gx", "gy", "gz"))
    index_section = lax.axis_index("section")
    me = index_gx * size_gy + index_gy
    micro_count = micro_inputs.shape[0]
    tokens = micro_inputs.shape[1] * size_gy
    features = micro_inputs.shape[2] * size_gx * size_gz
    slab = q_weight.shape[1]
    chunk = tokens // CHUNKS
    share = chunk // size_gz
    q_cols = q_weight.shape[2]
    kv_cols = kv_weight.shape[3]
    group_size = q_cols // kv_cols
    own_cols = q_cols // group
    own_heads = own_cols // HD
    used_heads = max(1, own_heads // group_size)
    used_cols = used_heads * HD
    width = own_cols + 2 * used_cols
    jobs = micro_count * CHUNKS

    offsets = [(dx, dy) for dx in range(size_gx) for dy in range(size_gy)][1:]
    offsets.sort(key=lambda o: (min(o[0], size_gx - o[0]) + min(o[1], size_gy - o[1])))

    def wrapped(index, step, size):
        moved = index + step
        return jnp.where(moved >= size, moved - size, moved)

    def cut_at(value, index, size):
        return lax.dynamic_slice_in_dim(value, index.astype(jnp.uint32), size, 0)

    def to_offset(value, dx, dy):
        pairs = [
            (x * size_gy + y, (x + dx) % size_gx * size_gy + (y + dy) % size_gy)
            for x in range(size_gx)
            for y in range(size_gy)
        ]
        return lax.ppermute(value, ("gx", "gy"), pairs)

    def kv_start(chip):
        if own_heads % group_size == 0:
            return chip * used_cols
        return chip * own_heads // group_size * HD

    even = size_gy == size_gz == CHUNKS
    if even:

        def spread(block):
            cut = block.reshape(size_gz, share, slab)
            pieces = []
            for j in range(CHUNKS):
                spot = wrapped(index_gy, j, size_gz)
                pairs = [
                    (a * size_gz + b, b * size_gz + (a + j) % size_gz) for a in range(size_gy) for b in range(size_gz)
                ]
                piece = cut_at(cut, spot, 1)[0]
                pieces.append(lax.ppermute(piece, ("gy", "gz"), pairs))
            return [
                sum_of([(index_gz == (k + j) % size_gz, pieces[j]) for j in range(CHUNKS)])
                for k in range(CHUNKS)
            ]

        def collect(found):
            sent = pick(table, range(picks, picks + CHUNKS), found)
            pieces = []
            for j in range(CHUNKS):
                pairs = [
                    (c * size_gz + d, (d + j) % size_gy * size_gz + c) for c in range(size_gy) for d in range(size_gz)
                ]
                pieces.append(lax.ppermute(sent[j], ("gy", "gz"), pairs))
            (rows,) = pick(table, range(picks + CHUNKS, picks + CHUNKS + size_gz), pieces, joined=True)
            return rows
    else:

        def spread(block):
            wide = gathered(block, "gz", 1)
            pieces = lax.all_to_all(wide, "gy", split_axis=1, concat_axis=0, tiled=True)
            pieces = pieces.reshape(CHUNKS, size_gz, share, slab)
            pieces = lax.dynamic_index_in_dim(pieces, index_gz, 1, keepdims=False)
            return [pieces[k] for k in range(CHUNKS)]

        def collect(found):
            slabs = [pick(table, [mine + 1], found[k : k + sections])[0] for k in range(CHUNKS)]
            rows = gathered(jnp.stack(slabs), "gz", 1).reshape(tokens, slab)
            wide = lax.all_to_all(rows, "gy", split_axis=0, concat_axis=1, tiled=True)
            piece = wide.shape[1] // size_gz
            return lax.dynamic_slice_in_dim(wide, index_gz * piece, piece, 1)

    def sum_of(choices):
        chosen = choices[0][1]
        for condition, value in choices[1:]:
            chosen = jnp.where(condition, value, chosen)
        return chosen

    gain_slab = cut_at(norm_gain[0], index_gy * slab, slab)[None, :]
    own_bias = jnp.concatenate(
        [
            cut_at(q_bias[0], me * own_cols, own_cols),
            cut_at(kv_bias[0, 0], kv_start(me), used_cols),
            cut_at(kv_bias[0, 1], kv_start(me), used_cols),
        ]
    )[None, :]

    order = (index_gz + jnp.arange(size_gz)) % size_gz
    row_pos = (order[:, None] * share + jnp.arange(share)[None, :]).reshape(chunk)
    half_width = HD // 2
    frequency = ROPE_BASE ** (-jnp.arange(half_width, dtype=jnp.float32) * 2.0 / HD)
    ticks = jobs + sections - 1
    ordinals = (jnp.arange(ticks) - index_section) % CHUNKS
    positions = ordinals[:, None] * chunk + row_pos[None, :]
    angles = positions.astype(jnp.float32)[:, :, None] * frequency[None, None, :]
    cosines = jnp.cos(angles)
    sines = jnp.sin(angles)
    cosines = list(jnp.concatenate([cosines, cosines], axis=-1))
    sines = list(jnp.concatenate([-sines, sines], axis=-1))
    causal = row_pos[None, :] <= row_pos[:, None]
    masks = [
        jnp.concatenate(
            [causal] + [jnp.broadcast_to(ordinals[t] >= j, (chunk, chunk)) for j in range(1, min(CHUNKS, t + 1))],
            axis=1,
        ).astype(jnp.float32)
        for t in range(ticks)
    ]
    far_first = offsets[::-1]
    square = size_gx == size_gy == 2
    steps_x = jnp.array([dx for dx, _ in far_first] + [-dx % size_gx for dx, _ in offsets] + [0], jnp.int32)
    steps_y = jnp.array([dy for _, dy in far_first] + [-dy % size_gy for _, dy in offsets] + [0], jnp.int32)
    chips = wrapped(index_gx, steps_x, size_gx) * size_gy + wrapped(index_gy, steps_y, size_gy)
    mine = 2 * len(offsets)
    choice = [jnp.stack([index_section, jnp.minimum(index_section, 1)])]
    picks = mine + 3
    if even:
        choice.append(wrapped(index_gz, jnp.arange(CHUNKS), size_gy) + index_section)
        choice.append(wrapped(index_gy, -jnp.arange(size_gz) % size_gz, size_gz))
    table = jnp.concatenate([chips, *choice]).astype(jnp.int32)
    early = [gain_slab, own_bias, *cosines, *sines, *masks]
    (table, early) = lax.optimization_barrier((table, early))
    gain_slab, own_bias = early[:2]
    cosines, sines, masks = (early[2 + i * ticks : 2 + (i + 1) * ticks] for i in range(3))
    entering = [piece for m in range(micro_count) for piece in spread(micro_inputs[m])]

    copies = []
    everything = slice(None)
    for chip in range(group):
        kv_from = chip * own_heads // group_size * HD
        target = (everything, pl.ds(chip * width, own_cols))
        copies.append((0, (0, everything, pl.ds(chip * own_cols, own_cols)), 0, target))
        for i in range(2):
            target = (everything, pl.ds(chip * width + own_cols + i * used_cols, used_cols))
            copies.append((1, (0, i, everything, pl.ds(kv_from, used_cols)), 0, target))
    kept = min(HELD_BLOCKS, len(offsets))
    held_copies = []
    for i in range(kept):
        slot = mine - 1 - i

        def where(table_ref, slot=slot):
            return 0, pl.ds(pl.multiple_of(table_ref[slot] * own_cols, 128), own_cols)

        held_copies.append((0, where, i, (everything,)))
    table, weights = resident([table], early, [q_weight, kv_weight], copies, [(slab, group * width)])
    _, *held = resident([table], [], [out_weight], held_copies, [(own_cols, slab)] * kept)
    held = {mine - 1 - i: w for i, w in enumerate(held)}
    mixing_weight = pltpu.with_memory_space_constraint(out_weight, pltpu.HBM)

    def layer(own_rows, tick, earlier):
        pieces = [own_rows] + [around(own_rows, "gz", -j) for j in range(1, size_gz)]
        scaled, total, *part = enter(table, 0, pieces, gain_slab, weights, width, 2 if square else 1)
        if square:
            from_x = to_offset(part[0], 1, 0)
            from_y = to_offset(part[1], 0, 1)
            later_y, near_y = project_block(table, 2, scaled, weights, width, jnp.bfloat16, 2)
            direct_y = to_offset(near_y, 0, 1)
            near_x, later_x = project_block(table, 1, scaled, weights, width, jnp.bfloat16, 2)
            direct_x = to_offset(near_x, 1, 0)
            to_y, to_x, total = fold(later_x, later_y, from_x, from_y, total)
            folded_y = to_offset(to_y, 0, 1)
            folded_x = to_offset(to_x, 1, 0)
            received = [[direct_x, folded_y], [direct_y, folded_x]]
            totals = [total]
        else:
            received = [[]]
            totals = [total]
            part = part[0]
            for k, o in enumerate(far_first):
                if k:
                    (part,) = project_block(table, k, scaled, weights, width, jnp.bfloat16)
                received[0].append(to_offset(part, *o))
            for o in far_first:
                totals.append(to_offset(total, *o))
        (projected,) = project_block(table, mine, scaled, weights, width, jnp.float32)
        *attended, keys, values = attend(
            projected,
            received,
            totals,
            own_bias,
            cosines[tick],
            sines[tick],
            masks[tick],
            earlier[: CHUNKS - 1],
            own_heads,
            used_heads,
            features,
        )
        seen = [(keys, values)] + earlier
        arrived = []
        if square:
            x_upper = to_offset(attended[0], 1, 0)
            y_lower = to_offset(attended[1], 0, 1)
            x_lower = to_offset(attended[1], 1, 0)
            y_upper = to_offset(attended[0], 0, 1)
            far_upper = to_offset(x_upper, 0, 1)
            far_lower = to_offset(y_lower, 1, 0)
            arrived = [(y_upper, y_lower), (x_upper, x_lower), (far_upper, far_lower)]
        else:
            for o in offsets:
                arrived.append((to_offset(attended[0], *o),))
        (sums,) = mix_blocks(table, [mine], [tuple(attended)], mixing_weight, held, None, 1)
        back = list(range(len(offsets), mine))
        if len(offsets) > 1:
            (sums,) = mix_blocks(table, back[:-1], arrived[:-1], mixing_weight, held, sums, 1)
        own_sum, *others = mix_blocks(table, back[-1:], arrived[-1:], mixing_weight, held, sums, size_gz)
        result = leave(own_rows, own_sum, [around(piece, "gz", j + 1) for j, piece in enumerate(others)])
        return result, seen

    results = []
    carried = None
    earlier = []
    for tick in range(ticks):
        if carried is None:
            current = entering[0]
        elif tick < jobs:
            (current,) = pick(table, [mine + 2], [entering[tick], carried])
        else:
            current = carried
        result, earlier = layer(current, tick, earlier)
        results.append(result)
        if tick < ticks - 1:
            carried = lax.ppermute(result, "section", [(i, i + 1) for i in range(sections - 1)])

    cuts = [results[m * CHUNKS : (m + 1) * CHUNKS + sections - 1] for m in range(micro_count)]
    return jnp.stack([collect(found) for found in cuts])[None]


def solution(mesh):
    return jax.shard_map(
        body,
        mesh=mesh,
        in_specs=(
            P(None, "gy", ("gx", "gz")),
            P("section", "gx"),
            P("section", ("gx", "gy"), "gz"),
            P("section", None, ("gx", "gy"), "gz"),
            P("section", "gz"),
            P("section", None, "gz"),
            P("section", "gz", ("gx", "gy")),
        ),
        out_specs=P("section", None, "gy", ("gx", "gz")),
        check_vma=False,
    )
```
